32 devices in a mesh: row: 4 (over z), col: 8 (over y, x, core).
Axes of the slice: x: 2, y: 2, z: 4, core: 2. Of those that a mesh axis runs over, the one named last changes fastest.
Arguments:
- features: bfloat16 [64, 131072], P(None, ('row', 'col')), may hold values from -6 to 6
- tile_rows: int32 [4, 8, 512], P('row', 'col'), may hold values from 0 to 255, as said below
- tile_cols: int32 [4, 8, 512], P('row', 'col'), may hold values from 0 to 127
- tile_count: int32 [4, 8], P('row', 'col'), may hold values from 1 to 512, as said below
- tile_data: bfloat16 [4, 8, 512, 128, 128], P('row', 'col'), may hold values from -0.21875 to 0.21875
Outputs:
- filtered: bfloat16 [512, 131072], P(None, ('row', 'col'))
The draws below stay inside these ranges and needn't reach their ends.
Inputs may be any that keep to these rules, and one draw needn't show every extreme that they name: Within one device the pairs (tile_rows, tile_cols) of all 512 slots are distinct. `tile_count`: some device has all 512 slots live in every draw.
All inputs are finite; a program needn't handle non-finite values.
Results may differ from the reference program's by a relative error of at most 0.009.
Values may be sent and summed in bfloat16 or wider, within the bound.
No kernel may reach another device: no remote copies, remote signals or barrier semaphores. Data moves between devices by JAX's collectives and lax.ppermute only.
A program may use at most 128 MiB of HBM per device.

```python
import jax
import jax.numpy as jnp
from jax import lax

CHANNELS = 64
SCALES = 8
TILE_SIZE = 128
NODES_DEV = 4096
TILES_MAX = 512
NODES = 131072
BLOCK_ROWS = 256
N_ROW = 4
N_COL = 8


def tile_cells(key):
    row_blocks = NODES_DEV * N_COL // TILE_SIZE
    col_blocks = NODES_DEV * N_ROW // TILE_SIZE
    keys = jax.random.split(jax.random.fold_in(key, 11), N_ROW * N_COL)

    def one_device(device_key):
        return jax.random.permutation(device_key, row_blocks * col_blocks)[:TILES_MAX]
    cells = jax.vmap(one_device)(keys)
    return (cells.reshape(N_ROW, N_COL, TILES_MAX).astype(jnp.int32), col_blocks)


def draw_tile_rows(key, part):
    cells, col_blocks = tile_cells(key)
    return (cells // col_blocks).astype(jnp.int32)


def draw_tile_cols(key, part):
    cells, col_blocks = tile_cells(key)
    return (cells % col_blocks).astype(jnp.int32)


def draw_tile_count(key, part):
    device_count = N_ROW * N_COL
    base_key = jax.random.fold_in(key, 23)
    full_key = jax.random.fold_in(key, 29)
    lowest = max(1, TILES_MAX // 8)
    highest = max(lowest + 1, TILES_MAX // 2 + 1)
    counts = jax.random.randint(base_key, (device_count,), lowest, highest).astype(jnp.int32)
    chosen = jax.random.permutation(full_key, device_count)[:max(1, device_count // 16)]
    counts = counts.at[chosen].set(TILES_MAX)
    return counts.reshape(N_ROW, N_COL).astype(jnp.int32)


def levels(key, shape, pieces, least, top_value):
    loudness, own = 1.0, jax.random.fold_in(key, 6)
    for axis_at, shards_of in pieces:
        draws = jnp.exp(jax.random.uniform(jax.random.fold_in(own, axis_at), (shards_of,), jnp.float32, least / len(pieces), top_value / len(pieces)))
        loudness = loudness * jnp.repeat(draws, shape[axis_at] // shards_of).reshape([-1 if axis == axis_at else 1 for axis in range(len(shape))])
    return loudness


def centred(stream_key, shape, deviation, bound, shards=(), kind=jnp.bfloat16):
    array = jax.random.normal(stream_key, shape, jnp.float32) * deviation
    if len(shards) > 0:
        array = levels(stream_key, shape, shards, -0.22, 0.18) * array
    return jnp.clip(array, min=-bound, max=bound).astype(kind)


def setup_inputs(seed: int = 0) -> dict:
    arg_keys = jax.random.split(jax.random.key(seed), 6)
    return {
        "features": centred(arg_keys[0], (CHANNELS, NODES), 1.0, 6.0, ((1, 32),)),
        "tile_rows": draw_tile_rows(jax.random.fold_in(arg_keys[5], 71), 0),
        "tile_cols": draw_tile_cols(jax.random.fold_in(arg_keys[5], 71), 0),
        "tile_count": draw_tile_count(jax.random.fold_in(arg_keys[5], 71), 0),
        "tile_data": centred(arg_keys[4], (N_ROW, N_COL, TILES_MAX, TILE_SIZE, TILE_SIZE), 768 ** -0.5, 0.21875, ((0, 4), (1, 8))),
    }


def bessel_pair(times):
    halved = times / 2.0
    square = halved * halved
    term_zero = jnp.ones_like(times)
    term_one = halved
    sum_zero = term_zero
    sum_one = term_one
    for degree in range(1, 24):
        term_zero = term_zero * square / float(degree * degree)
        term_one = term_one * square / float(degree * (degree + 1))
        sum_zero = sum_zero + term_zero
        sum_one = sum_one + term_one
    damping = jnp.exp(-times)
    return damping * sum_zero, damping * sum_one


def coefficients():
    times = 0.25 * 2.0 ** (jnp.arange(SCALES).astype(jnp.float32) / 2.0)
    bessel_zero, bessel_one = bessel_pair(times)
    return bessel_zero, -2.0 * bessel_one, 2.0 * (bessel_zero - 2.0 * bessel_one / times)


def apply_operator(field, tile_rows, tile_cols, tile_count, tile_data):
    per_block = NODES_DEV // TILE_SIZE
    blocks = field.reshape(CHANNELS, NODES // TILE_SIZE, TILE_SIZE)
    device_count = N_ROW * N_COL
    slot_rows = tile_rows.reshape(device_count, TILES_MAX)
    slot_cols = tile_cols.reshape(device_count, TILES_MAX)
    slot_live = tile_count.reshape(device_count)
    slot_data = tile_data.reshape(device_count, TILES_MAX, TILE_SIZE, TILE_SIZE)

    def one_device(summed, inputs):
        row_ids, col_ids, live_count, entries, device = inputs
        row_group = device // N_COL
        col_group = device % N_COL
        global_cols = ((col_ids // per_block) * N_COL + col_group) * per_block + col_ids % per_block
        picked = jnp.take(blocks, global_cols.astype(jnp.int32), axis=1)
        product = jnp.einsum("fgk,grk->fgr", picked.astype(jnp.float32), entries.astype(jnp.float32))
        live = (jnp.arange(TILES_MAX) < live_count).astype(jnp.float32)
        product = product * live[None, :, None]
        partial_value = jnp.zeros((CHANNELS, BLOCK_ROWS, TILE_SIZE), jnp.float32).at[:, row_ids].add(product)
        partial_value = partial_value.astype(jnp.bfloat16).astype(jnp.float32)
        offset = (row_group * BLOCK_ROWS).astype(jnp.int32)
        current = lax.dynamic_slice_in_dim(summed, offset, BLOCK_ROWS, 1)
        summed = lax.dynamic_update_slice_in_dim(summed, current + partial_value, offset, 1)
        return summed, None

    start = jnp.zeros((CHANNELS, NODES // TILE_SIZE, TILE_SIZE), jnp.float32)
    device_ids = jnp.arange(device_count).astype(jnp.int32)
    summed, _ = lax.scan(one_device, start, (slot_rows, slot_cols, slot_live, slot_data, device_ids))
    return summed.reshape(CHANNELS, NODES).astype(jnp.bfloat16)


def reference(features, tile_rows, tile_cols, tile_count, tile_data):
    first = apply_operator(features, tile_rows, tile_cols, tile_count, tile_data)
    second = apply_operator(first, tile_rows, tile_cols, tile_count, tile_data)
    coef_zero, coef_one, coef_two = coefficients()
    base = features.astype(jnp.float32)
    first_wide = first.astype(jnp.float32)
    second_wide = second.astype(jnp.float32)
    filtered = (coef_zero[:, None, None] * base[None] + coef_one[:, None, None] * first_wide[None]
                + coef_two[:, None, None] * (2.0 * second_wide - base)[None])
    return filtered.reshape(SCALES * CHANNELS, NODES).astype(jnp.bfloat16)
```

```python
import functools

import jax
import jax.numpy as jnp
from jax import lax
from jax.experimental import pallas as pl
from jax.experimental.pallas import tpu as pltpu
from jax.sharding import PartitionSpec as P

SCALES = 8
TILE_SIZE = 128
CHUNKS = 2
GROUP = 16


def bessel_pair(times):
    halved = times / 2.0
    square = halved * halved
    term_zero = jnp.ones_like(times)
    term_one = halved
    sum_zero = term_zero
    sum_one = term_one
    for degree in range(1, 24):
        term_zero = term_zero * square / float(degree * degree)
        term_one = term_one * square / float(degree * (degree + 1))
        sum_zero = sum_zero + term_zero
        sum_one = sum_one + term_one
    damping = jnp.exp(-times)
    return (damping * sum_zero, damping * sum_one)


def coefficients():
    times = 0.25 * 2.0 ** (jnp.arange(SCALES).astype(jnp.float32) / 2.0)
    bessel_zero, bessel_one = bessel_pair(times)
    return (bessel_zero, -2.0 * bessel_one, 2.0 * (bessel_zero - 2.0 * bessel_one / times))


def tile_kernel(pieces, halves, place_ref, rows_ref, cols_ref, tiles_ref, *refs):
    piece_refs = refs[:pieces]
    keep_ref, send_ref = refs[pieces : pieces + 2]
    panel_ref, acc_ref, sems = refs[pieces + 2 :]
    step = pl.program_id(0)
    group = tiles_ref.shape[0]
    per_dev = panel_ref.shape[2] // TILE_SIZE
    count = place_ref[0]

    @pl.when(step == 0)
    def _():
        copies = [
            pltpu.make_async_copy(piece_refs[i], panel_ref.at[i], sems.at[i])
            for i in range(pieces)
        ]
        for copy in copies:
            copy.start()

        @pl.loop(0, acc_ref.shape[0])
        def _(row):
            acc_ref[row] = jnp.zeros(acc_ref.shape[1:], jnp.float32)

        for copy in copies:
            copy.wait()

    @pl.when(step * group < count)
    def _():
        for g in range(group):
            slot = step * group + g
            col = cols_ref[slot]
            row = rows_ref[slot]
            offset = pl.multiple_of((col % per_dev) * TILE_SIZE, TILE_SIZE)
            picked = panel_ref[col // per_dev, :, pl.ds(offset, TILE_SIZE)]
            product = lax.dot_general(
                picked, tiles_ref[g], (((1,), (1,)), ((), ())),
                preferred_element_type=jnp.float32,
            )
            acc_ref[row] += product

    @pl.when(step == pl.num_programs(0) - 1)
    def _():
        pair = place_ref[1]
        core = place_ref[2]

        @pl.loop(0, halves)
        def _(h):
            base = (pair ^ h) * 2
            for ref, side in ((keep_ref, core), (send_ref, 1 - core)):
                start = (base + side) * per_dev
                for j in range(per_dev):
                    ref[h, :, j * TILE_SIZE : (j + 1) * TILE_SIZE] = acc_ref[start + j].astype(
                        jnp.bfloat16
                    )


def tile_products(parts, place, slot_rows, slot_cols, slot_data, block_rows, halves):
    channels, nodes = parts[0].shape
    slots = slot_rows.shape[0]
    group = min(GROUP, slots)
    pieces = len(parts)

    def tile_block(step, place_ref, rows_ref, cols_ref):
        last = jnp.maximum(place_ref[0] - 1, 0) // group
        return (jnp.minimum(step, last), 0, 0)

    def whole(step, *_):
        return (0, 0, 0)

    out = jax.ShapeDtypeStruct((halves, channels, nodes), jnp.bfloat16)
    return pl.pallas_call(
        functools.partial(tile_kernel, pieces, halves),
        grid_spec=pltpu.PrefetchScalarGridSpec(
            num_scalar_prefetch=3,
            grid=(slots // group,),
            in_specs=[pl.BlockSpec((group, TILE_SIZE, TILE_SIZE), tile_block)]
            + [pl.BlockSpec(memory_space=pl.ANY)] * pieces,
            out_specs=[pl.BlockSpec((halves, channels, nodes), whole)] * 2,
            scratch_shapes=[
                pltpu.VMEM((pieces, channels, nodes), jnp.bfloat16),
                pltpu.VMEM((block_rows + 1, channels, TILE_SIZE), jnp.float32),
                pltpu.SemaphoreType.DMA((pieces,)),
            ],
        ),
        out_shape=[out, out],
        cost_estimate=pl.CostEstimate(
            flops=2 * slots * channels * TILE_SIZE * TILE_SIZE * 8,
            bytes_accessed=slots * TILE_SIZE * TILE_SIZE * 2,
            transcendentals=0,
        ),
    )(place, slot_rows, slot_cols, slot_data, *parts)


def flip(size, mask):
    return [(i, i ^ mask) for i in range(size)]


def gather_parts(own, rows):
    if rows == 4:
        far = lax.ppermute(own, "row", flip(rows, 2))
        near = lax.ppermute(own, "row", flip(rows, 1))
        inner = lax.ppermute(own, "row", [(1, 2), (2, 1)])
        outer = lax.ppermute(far, "row", [(2, 3), (1, 0)])
        row = lax.axis_index("row")
        inside = (row == 1) | (row == 2)
        return [own, near, far, jnp.where(inside, inner, outer)]
    return [own] + [lax.ppermute(own, "row", flip(rows, mask)) for mask in range(1, rows)]


def reduce_parts(keep, send, cols):
    arrived = lax.ppermute(send, "col", flip(cols, 1))
    paired = (keep.astype(jnp.float32) + arrived.astype(jnp.float32)).astype(jnp.bfloat16)
    total = paired[0].astype(jnp.float32)
    for half in range(1, cols // 2):
        total = total + lax.ppermute(paired[half], "col", flip(cols, 2 * half)).astype(jnp.float32)
    return total.astype(jnp.bfloat16)


def shards(features, tile_rows, tile_cols, tile_count, tile_data):
    cols = lax.axis_size("col")
    rows = lax.axis_size("row")
    channels, nodes = features.shape
    per_dev = nodes // TILE_SIZE
    block_rows = per_dev * cols
    slot_data = tile_data.reshape(-1, TILE_SIZE, TILE_SIZE)
    slots = slot_data.shape[0]
    live = tile_count.reshape(())
    row_at, col_at = lax.axis_index("row"), lax.axis_index("col")
    slot_rows = jnp.where(jnp.arange(slots) < live, tile_rows.reshape(-1), block_rows)
    slot_cols = tile_cols.reshape(-1)
    slot_cols = ((slot_cols // per_dev) ^ row_at) * per_dev + slot_cols % per_dev
    place = jnp.stack([live, col_at // 2, col_at % 2]).astype(jnp.int32)

    def apply_operator(field):
        keep, send = tile_products(
            gather_parts(field, rows), place, slot_rows, slot_cols, slot_data, block_rows, cols // 2
        )
        return reduce_parts(keep, send, cols)

    width = channels // CHUNKS
    coef_zero, coef_one, coef_two = coefficients()
    outs = []
    fields = [features[i * width : (i + 1) * width] for i in range(CHUNKS)]
    firsts = [apply_operator(field) for field in fields]
    seconds = [apply_operator(first) for first in firsts]
    for field, first, second in zip(fields, firsts, seconds):
        base = field.astype(jnp.float32)
        first_wide = first.astype(jnp.float32)
        second_wide = second.astype(jnp.float32)
        outs.append(
            (
                coef_zero[:, None, None] * base[None]
                + coef_one[:, None, None] * first_wide[None]
                + coef_two[:, None, None] * (2.0 * second_wide - base)[None]
            ).astype(jnp.bfloat16)
        )
    return jnp.concatenate(outs, axis=1).reshape(-1, nodes)


def solution(mesh):
    return jax.shard_map(
        shards,
        mesh=mesh,
        in_specs=(
            P(None, ("row", "col")),
            P("row", "col", None),
            P("row", "col", None),
            P("row", "col"),
            P("row", "col", None, None, None),
        ),
        out_specs=P(None, ("row", "col")),
        check_vma=False,
    )
```

```python
import functools

import jax
import jax.numpy as jnp
from jax import lax
from jax.experimental import pallas as pl
from jax.experimental.pallas import tpu as pltpu
from jax.sharding import PartitionSpec as P


SCALES = 8
TILE_SIZE = 128
CHUNKS = 2
GROUP = 64
FLIP_GROUP = 16


def bessel_pair(times):
    halved = times / 2.0
    square = halved * halved
    term_zero = jnp.ones_like(times)
    term_one = halved
    sum_zero = term_zero
    sum_one = term_one
    for degree in range(1, 24):
        term_zero = term_zero * square / float(degree * degree)
        term_one = term_one * square / float(degree * (degree + 1))
        sum_zero = sum_zero + term_zero
        sum_one = sum_one + term_one
    damping = jnp.exp(-times)
    return (damping * sum_zero, damping * sum_one)


def coefficients():
    times = 0.25 * 2.0 ** (jnp.arange(SCALES).astype(jnp.float32) / 2.0)
    bessel_zero, bessel_one = bessel_pair(times)
    return (bessel_zero, -2.0 * bessel_one, 2.0 * (bessel_zero - 2.0 * bessel_one / times))


def flip_kernel(group, first, place_ref, tiles_hbm, out_hbm, tiles_ref, flipped_ref, in_sems, out_sems):
    slots = tiles_ref.shape[0]
    live = jnp.clip(place_ref[0] - first, 0, slots)
    live_groups = lax.div(live + (group - 1), group)

    def load(index):
        source = tiles_hbm.at[pl.ds(first + index * group, group)]
        target = tiles_ref.at[pl.ds(index * group, group)]
        return pltpu.make_async_copy(source, target, in_sems.at[index])

    def save(index):
        span = pl.ds(index * group, group)
        return pltpu.make_async_copy(flipped_ref.at[span], out_hbm.at[span], out_sems.at[index])

    @pl.loop(0, live_groups)
    def _(index):
        load(index).start()

    @pl.loop(0, live_groups)
    def _(index):
        load(index).wait()
        for g in range(group):
            slot = index * group + g
            flipped_ref[slot] = tiles_ref[slot].T
        save(index).start()

    @pl.loop(0, live_groups)
    def _(index):
        save(index).wait()


def flip_tiles(place, slot_data, first, slots):
    group = min(FLIP_GROUP, slots)
    anywhere = pl.BlockSpec(memory_space=pl.ANY)
    shape = (slots, TILE_SIZE, TILE_SIZE)
    return pl.pallas_call(
        functools.partial(flip_kernel, group, first),
        in_specs=[pl.BlockSpec(memory_space=pltpu.SMEM), anywhere],
        out_specs=anywhere,
        scratch_shapes=[
            pltpu.VMEM(shape, jnp.bfloat16),
            pltpu.VMEM(shape, jnp.bfloat16),
            pltpu.SemaphoreType.DMA((slots // group,)),
            pltpu.SemaphoreType.DMA((slots // group,)),
        ],
        out_shape=jax.ShapeDtypeStruct(shape, jnp.bfloat16),
        cost_estimate=pl.CostEstimate(
            flops=2 * slots * TILE_SIZE**3,
            bytes_accessed=slots * TILE_SIZE * TILE_SIZE * 4,
            transcendentals=0,
        ),
    )(place, slot_data)


def tile_kernel(pieces, group, place_ref, rows_ref, cols_ref, tiles_low, tiles_high, *refs):
    piece_refs = refs[:pieces]
    keep_hbm, send_hbm = refs[pieces : pieces + 2]
    tiles_ref, panel_ref, acc_ref, keep_ref, send_ref, piece_sems, tile_sems, out_sems = refs[
        pieces + 2 :
    ]
    halves = keep_ref.shape[0]
    per_dev = panel_ref.shape[2] // TILE_SIZE
    live_groups = lax.div(place_ref[0] + (group - 1), group)
    low_groups = tiles_low.shape[0] // group

    def tile_copy(tiles_hbm, base, index):
        return pltpu.make_async_copy(
            tiles_hbm.at[pl.ds((index - base) * group, group)],
            tiles_ref.at[pl.ds(index * group, group)],
            tile_sems.at[index],
        )

    copies = [
        pltpu.make_async_copy(piece_refs[i], panel_ref.at[i], piece_sems.at[i])
        for i in range(pieces)
    ]
    for copy in copies:
        copy.start()

    @pl.loop(0, jnp.minimum(live_groups, low_groups))
    def _(index):
        tile_copy(tiles_low, 0, index).start()

    @pl.loop(low_groups, jnp.maximum(live_groups, low_groups))
    def _(index):
        tile_copy(tiles_high, low_groups, index).start()

    @pl.loop(0, acc_ref.shape[0] // 8)
    def _(index):
        acc_ref[pl.ds(index * 8, 8)] = jnp.zeros((8,) + acc_ref.shape[1:], jnp.float32)

    for copy in copies:
        copy.wait()

    @pl.loop(0, live_groups)
    def _(index):
        tile_copy(tiles_low, index, index).wait()
        for g in range(group):
            slot = index * group + g
            col = cols_ref[slot]
            row = rows_ref[slot]
            offset = pl.multiple_of((col & (per_dev - 1)) * TILE_SIZE, TILE_SIZE)
            picked = panel_ref[lax.div(col, per_dev), :, pl.ds(offset, TILE_SIZE)]
            product = lax.dot_general(
                picked, tiles_ref[slot], (((1,), (0,)), ((), ())),
                preferred_element_type=jnp.float32,
            )
            acc_ref[row] += product

    pair = place_ref[1]
    core = place_ref[2]

    def out_copies(h):
        return (
            pltpu.make_async_copy(send_ref.at[h], send_hbm.at[h], out_sems.at[0, h]),
            pltpu.make_async_copy(keep_ref.at[h], keep_hbm.at[h], out_sems.at[1, h]),
        )

    @pl.loop(0, halves)
    def _(h):
        base = (pair ^ h) * 2
        send_copy, keep_copy = out_copies(h)
        for ref, side, copy in ((send_ref, 1 - core, send_copy), (keep_ref, core, keep_copy)):
            start = (base + side) * per_dev
            for j in range(per_dev):
                ref[h, :, j * TILE_SIZE : (j + 1) * TILE_SIZE] = acc_ref[start + j].astype(
                    jnp.bfloat16
                )
            copy.start()

    @pl.loop(0, halves)
    def _(h):
        for copy in out_copies(h):
            copy.wait()


def tile_products(parts, place, slot_rows, slot_cols, tiles, block_rows, halves):
    channels, nodes = parts[0].shape
    slots = slot_rows.shape[0]
    group = min(GROUP, slots)
    pieces = len(parts)
    out = jax.ShapeDtypeStruct((halves, channels, nodes), jnp.bfloat16)
    anywhere = pl.BlockSpec(memory_space=pl.ANY)
    scalars = pl.BlockSpec(memory_space=pltpu.SMEM)
    return pl.pallas_call(
        functools.partial(tile_kernel, pieces, group),
        in_specs=[scalars] * 3 + [anywhere] * (2 + pieces),
        out_specs=[anywhere] * 2,
        scratch_shapes=[
            pltpu.VMEM((slots, TILE_SIZE, TILE_SIZE), jnp.bfloat16),
            pltpu.VMEM((pieces, channels, nodes), jnp.bfloat16),
            pltpu.VMEM((block_rows + 8, channels, TILE_SIZE), jnp.float32),
            pltpu.VMEM((halves, channels, nodes), jnp.bfloat16),
            pltpu.VMEM((halves, channels, nodes), jnp.bfloat16),
            pltpu.SemaphoreType.DMA((pieces,)),
            pltpu.SemaphoreType.DMA((slots // group,)),
            pltpu.SemaphoreType.DMA((2, halves)),
        ],
        out_shape=[out, out],
        cost_estimate=pl.CostEstimate(
            flops=2 * slots * channels * TILE_SIZE * TILE_SIZE * 8,
            bytes_accessed=slots * TILE_SIZE * TILE_SIZE * 2,
            transcendentals=0,
        ),
    )(place, slot_rows, slot_cols, *tiles, *parts)


def flip(size, mask):
    return [(i, i ^ mask) for i in range(size)]


def gather_parts(own, rows):
    def send(value, pairs):
        return lax.ppermute(value, "row", pairs)

    if rows == 4:
        far = send(own, flip(rows, 2))
        near = send(own, flip(rows, 1))
        inner = send(own, [(1, 2), (2, 1)])
        outer = send(far, [(2, 3), (1, 0)])
        return [own, near, far, inner, outer]
    return [own] + [send(own, flip(rows, mask)) for mask in range(1, rows)]


def reduce_parts(keep, send, cols):
    arrived = lax.ppermute(send, "col", flip(cols, 1))
    paired = [
        (keep[half].astype(jnp.float32) + arrived[half].astype(jnp.float32)).astype(jnp.bfloat16)
        for half in range(cols // 2)
    ]
    terms = [paired[0]]
    for half in range(1, cols // 2):
        terms.append(lax.ppermute(paired[half], "col", flip(cols, 2 * half)))
    total = terms[0].astype(jnp.float32)
    for term in terms[1:]:
        total = total + term.astype(jnp.float32)
    return total.astype(jnp.bfloat16)


def filter_bank(features, tile_rows, tile_cols, tile_count, tile_data):
    cols = lax.axis_size("col")
    rows = lax.axis_size("row")
    channels, nodes = features.shape
    per_dev = nodes // TILE_SIZE
    block_rows = per_dev * cols
    slot_data = tile_data.reshape(-1, TILE_SIZE, TILE_SIZE)
    slots = slot_data.shape[0]
    live = tile_count.reshape(())
    row_at, col_at = lax.axis_index("row"), lax.axis_index("col")
    slot_rows = jnp.where(jnp.arange(slots) < live, tile_rows.reshape(-1), block_rows)
    slot_cols = tile_cols.reshape(-1)
    source = (slot_cols // per_dev) ^ row_at
    if rows == 4:
        source = source + ((source == 3) & ((row_at == 0) | (row_at == 3))).astype(jnp.int32)
    slot_cols = source * per_dev + slot_cols % per_dev
    place = jnp.stack([live, col_at // 2, col_at % 2]).astype(jnp.int32)

    low = slots // 2
    tiles = []
    for begin, size in ((0, low), (low, slots - low)):
        tiles.append(flip_tiles(place, slot_data, begin, size))

    def apply_operator(field):
        parts = gather_parts(field, rows)
        keep, send = tile_products(parts, place, slot_rows, slot_cols, tiles, block_rows, cols // 2)
        return reduce_parts(keep, send, cols)

    width = channels // CHUNKS
    coef_zero, coef_one, coef_two = coefficients()
    outs = []
    fields = [features[i * width : (i + 1) * width] for i in range(CHUNKS)]
    firsts = [apply_operator(field) for field in fields]
    seconds = [apply_operator(first) for first in firsts]
    for field, first, second in zip(fields, firsts, seconds):
        base = field.astype(jnp.float32)
        first_wide = first.astype(jnp.float32)
        second_wide = second.astype(jnp.float32)
        outs.append(
            (
                coef_zero[:, None, None] * base[None]
                + coef_one[:, None, None] * first_wide[None]
                + coef_two[:, None, None] * (2.0 * second_wide - base)[None]
            ).astype(jnp.bfloat16)
        )
    return jnp.concatenate(outs, axis=1).reshape(-1, nodes)


def solution(mesh):
    return jax.shard_map(
        filter_bank,
        mesh=mesh,
        in_specs=(
            P(None, ("row", "col")),
            P("row", "col", None),
            P("row", "col", None),
            P("row", "col"),
            P("row", "col", None, None, None),
        ),
        out_specs=P(None, ("row", "col")),
        check_vma=False,
    )
```

```python
import functools

import jax
import jax.numpy as jnp
from jax import lax
from jax.experimental import pallas as pl
from jax.experimental.pallas import tpu as pltpu
from jax.sharding import PartitionSpec as P


SCALES = 8
TILE_SIZE = 128
CHUNKS = 2
GROUP = 64
FLIP_GROUP = 32
FLIP_DEPTH = 8
FLIP_VMEM = 28 * 2**20
SPARE_VMEM = 24 * 2**20


def bessel_pair(times):
    halved = times / 2.0
    square = halved * halved
    term_zero = jnp.ones_like(times)
    term_one = halved
    sum_zero = term_zero
    sum_one = term_one
    for degree in range(1, 24):
        term_zero = term_zero * square / float(degree * degree)
        term_one = term_one * square / float(degree * (degree + 1))
        sum_zero = sum_zero + term_zero
        sum_one = sum_one + term_one
    damping = jnp.exp(-times)
    return (damping * sum_zero, damping * sum_one)


def coefficients():
    times = 0.25 * 2.0 ** (jnp.arange(SCALES).astype(jnp.float32) / 2.0)
    bessel_zero, bessel_one = bessel_pair(times)
    return (bessel_zero, -2.0 * bessel_one, 2.0 * (bessel_zero - 2.0 * bessel_one / times))


def flip_kernel(group, depth, count_ref, tiles_hbm, flipped_ref, tiles_ref, sems):
    live_groups = lax.div(count_ref[0] + (group - 1), group)

    def load(index):
        slot = lax.rem(index, depth)
        source = tiles_hbm.at[pl.ds(index * group, group)]
        return pltpu.make_async_copy(source, tiles_ref.at[slot], sems.at[slot])

    for index in range(depth):

        @pl.when(index < live_groups)
        def _():
            load(index).start()

    @pl.loop(0, live_groups)
    def _(index):
        load(index).wait()
        for g in range(group):
            flipped_ref[index * group + g] = tiles_ref[lax.rem(index, depth), g].T

        @pl.when(index + depth < live_groups)
        def _():
            load(index + depth).start()


def flip_tiles(live, slot_data):
    slots = slot_data.shape[0]
    group = min(FLIP_GROUP, slots)
    depth = min(FLIP_DEPTH, slots // group)
    return pl.pallas_call(
        functools.partial(flip_kernel, group, depth),
        in_specs=[pl.BlockSpec(memory_space=pltpu.SMEM), pl.BlockSpec(memory_space=pl.ANY)],
        out_specs=pl.BlockSpec(memory_space=pltpu.VMEM),
        scratch_shapes=[
            pltpu.VMEM((depth, group, TILE_SIZE, TILE_SIZE), jnp.bfloat16),
            pltpu.SemaphoreType.DMA((depth,)),
        ],
        out_shape=jax.ShapeDtypeStruct(slot_data.shape, jnp.bfloat16),
        compiler_params=pltpu.CompilerParams(vmem_limit_bytes=FLIP_VMEM),
        cost_estimate=pl.CostEstimate(
            flops=slots * TILE_SIZE**3,
            bytes_accessed=slots * TILE_SIZE * TILE_SIZE * 2,
            transcendentals=0,
        ),
    )(live, slot_data)


def tile_kernel(pieces, group, count_ref, rows_ref, cols_ref, tiles_ref, *refs):
    piece_refs = refs[:pieces]
    keep_ref, send_ref = refs[pieces : pieces + 2]
    panel_ref, acc_ref, piece_sems = refs[pieces + 2 :]
    halves = keep_ref.shape[0]
    per_dev = panel_ref.shape[2] // TILE_SIZE
    count = count_ref[0]
    row_at = lax.axis_index("row")
    col_at = lax.axis_index("col")
    trash = acc_ref.shape[0] - 1
    shifted = pieces - 1 if pieces != lax.axis_size("row") else None
    at_end = (row_at == 0) | (row_at == lax.axis_size("row") - 1)

    copies = [
        pltpu.make_async_copy(piece_refs[i], panel_ref.at[i], piece_sems.at[i])
        for i in range(pieces)
    ]
    for copy in copies:
        copy.start()

    @pl.loop(0, acc_ref.shape[0] // 8)
    def _(index):
        acc_ref[pl.ds(index * 8, 8)] = jnp.zeros((8,) + acc_ref.shape[1:], jnp.float32)

    for copy in copies:
        copy.wait()

    @pl.loop(0, lax.div(count + (group - 1), group))
    def _(index):
        for g in range(group):
            slot = index * group + g
            col = cols_ref[slot]
            row = jnp.where(slot < count, rows_ref[slot], trash)
            source = lax.div(col, per_dev) ^ row_at
            if shifted is not None:
                source = jnp.where(at_end & (source == shifted - 1), shifted, source)
            offset = pl.multiple_of((col & (per_dev - 1)) * TILE_SIZE, TILE_SIZE)
            picked = panel_ref[source, :, pl.ds(offset, TILE_SIZE)]
            acc_ref[row] += jnp.dot(picked, tiles_ref[slot], preferred_element_type=jnp.float32)

    pair = lax.div(col_at, 2)
    core = col_at & 1

    @pl.loop(0, halves)
    def _(h):
        base = (pair ^ h) * 2
        for ref, side in ((send_ref, 1 - core), (keep_ref, core)):
            start = (base + side) * per_dev
            for j in range(per_dev):
                ref[h, :, j * TILE_SIZE : (j + 1) * TILE_SIZE] = acc_ref[start + j].astype(
                    jnp.bfloat16
                )


def tile_products(parts, live, slot_rows, slot_cols, tiles, block_rows, halves):
    channels, nodes = parts[0].shape
    slots = slot_rows.shape[0]
    group = min(GROUP, slots)
    pieces = len(parts)
    out = jax.ShapeDtypeStruct((halves, channels, nodes), jnp.bfloat16)
    scalars = pl.BlockSpec(memory_space=pltpu.SMEM)
    vectors = pl.BlockSpec(memory_space=pltpu.VMEM)
    scratch = channels * (4 * (block_rows + 8) * TILE_SIZE + 2 * pieces * nodes)
    return pl.pallas_call(
        functools.partial(tile_kernel, pieces, group),
        in_specs=[scalars] * 3 + [vectors] + [pl.BlockSpec(memory_space=pl.ANY)] * pieces,
        out_specs=[vectors] * 2,
        scratch_shapes=[
            pltpu.VMEM((pieces, channels, nodes), jnp.bfloat16),
            pltpu.VMEM((block_rows + 8, channels, TILE_SIZE), jnp.float32),
            pltpu.SemaphoreType.DMA((pieces,)),
        ],
        out_shape=[out, out],
        compiler_params=pltpu.CompilerParams(vmem_limit_bytes=scratch + SPARE_VMEM),
        cost_estimate=pl.CostEstimate(
            flops=2 * slots * channels * TILE_SIZE * TILE_SIZE * 8,
            bytes_accessed=slots * TILE_SIZE * TILE_SIZE * 2,
            transcendentals=0,
        ),
    )(live, slot_rows, slot_cols, tiles, *parts)


def flip(size, mask):
    return [(i, i ^ mask) for i in range(size)]


def gather_parts(own, rows):
    def send(value, pairs):
        return lax.ppermute(value, "row", pairs)

    if rows == 4:
        far = send(own, flip(rows, 2))
        near = send(own, flip(rows, 1))
        inner = send(own, [(1, 2), (2, 1)])
        outer = send(far, [(2, 3), (1, 0)])
        return [own, near, far, inner, outer]
    return [own] + [send(own, flip(rows, mask)) for mask in range(1, rows)]


def reduce_parts(keep, send, cols):
    arrived = lax.ppermute(send, "col", flip(cols, 1))
    paired = [
        (keep[half].astype(jnp.float32) + arrived[half].astype(jnp.float32)).astype(jnp.bfloat16)
        for half in range(cols // 2)
    ]
    terms = [paired[0]]
    for half in range(1, cols // 2):
        terms.append(lax.ppermute(paired[half], "col", flip(cols, 2 * half)))
    total = terms[0].astype(jnp.float32)
    for term in terms[1:]:
        total = total + term.astype(jnp.float32)
    return total.astype(jnp.bfloat16)


def filter_bank(features, tile_rows, tile_cols, tile_count, tile_data):
    cols = lax.axis_size("col")
    rows = lax.axis_size("row")
    channels, nodes = features.shape
    per_dev = nodes // TILE_SIZE
    block_rows = per_dev * cols
    slot_data = tile_data.reshape(-1, TILE_SIZE, TILE_SIZE)
    live = tile_count.reshape(-1)
    slot_rows = tile_rows.reshape(-1)
    slot_cols = tile_cols.reshape(-1)

    tiles = flip_tiles(live, slot_data)

    def apply_operator(field):
        parts = gather_parts(field, rows)
        keep, send = tile_products(parts, live, slot_rows, slot_cols, tiles, block_rows, cols // 2)
        return reduce_parts(keep, send, cols)

    width = channels // CHUNKS
    coef_zero, coef_one, coef_two = coefficients()
    fields = [features[i * width : (i + 1) * width] for i in range(CHUNKS)]
    firsts = [apply_operator(field) for field in fields]
    seconds = [apply_operator(first) for first in firsts]
    filtered = jnp.zeros((SCALES, channels, nodes), jnp.bfloat16)
    for chunk, (field, first, second) in enumerate(zip(fields, firsts, seconds)):
        base = field.astype(jnp.float32)
        first_wide = first.astype(jnp.float32)
        second_wide = second.astype(jnp.float32)
        block = (
            coef_zero[:, None, None] * base[None]
            + coef_one[:, None, None] * first_wide[None]
            + coef_two[:, None, None] * (2.0 * second_wide - base)[None]
        ).astype(jnp.bfloat16)
        filtered = lax.dynamic_update_slice(filtered, block, (0, chunk * width, 0))
    return filtered.reshape(-1, nodes)


def solution(mesh):
    return jax.shard_map(
        filter_bank,
        mesh=mesh,
        in_specs=(
            P(None, ("row", "col")),
            P("row", "col", None),
            P("row", "col", None),
            P("row", "col"),
            P("row", "col", None, None, None),
        ),
        out_specs=P(None, ("row", "col")),
        check_vma=False,
    )
```

```python
import functools

import jax
import jax.numpy as jnp
from jax import lax
from jax.experimental import pallas as pl
from jax.experimental.pallas import tpu as pltpu
from jax.sharding import PartitionSpec as P


SCALES = 8
TILE_SIZE = 128
CHUNKS = 2
GROUP = 64
FLIP_GROUP = 32
FLIP_DEPTH = 8
FLIP_VMEM = 28 * 2**20
SPARE_VMEM = 24 * 2**20
FILTER_VMEM = 16 * 2**20


def bessel_pair(times):
    halved = times / 2.0
    square = halved * halved
    term_zero = jnp.ones_like(times)
    term_one = halved
    sum_zero = term_zero
    sum_one = term_one
    for degree in range(1, 24):
        term_zero = term_zero * square / float(degree * degree)
        term_one = term_one * square / float(degree * (degree + 1))
        sum_zero = sum_zero + term_zero
        sum_one = sum_one + term_one
    damping = jnp.exp(-times)
    return (damping * sum_zero, damping * sum_one)


def coefficients():
    times = 0.25 * 2.0 ** (jnp.arange(SCALES).astype(jnp.float32) / 2.0)
    bessel_zero, bessel_one = bessel_pair(times)
    return (bessel_zero, -2.0 * bessel_one, 2.0 * (bessel_zero - 2.0 * bessel_one / times))


def flip_kernel(group, depth, count_ref, tiles_hbm, flipped_ref, tiles_ref, sems):
    live_groups = lax.div(count_ref[0] + (group - 1), group)

    def load(index):
        slot = lax.rem(index, depth)
        source = tiles_hbm.at[pl.ds(index * group, group)]
        return pltpu.make_async_copy(source, tiles_ref.at[slot], sems.at[slot])

    for index in range(depth):

        @pl.when(index < live_groups)
        def _():
            load(index).start()

    @pl.loop(0, live_groups)
    def _(index):
        load(index).wait()
        for g in range(group):
            flipped_ref[index * group + g] = tiles_ref[lax.rem(index, depth), g].T

        @pl.when(index + depth < live_groups)
        def _():
            load(index + depth).start()


def flip_tiles(live, slot_data):
    slots = slot_data.shape[0]
    group = min(FLIP_GROUP, slots)
    depth = min(FLIP_DEPTH, slots // group)
    return pl.pallas_call(
        functools.partial(flip_kernel, group, depth),
        in_specs=[pl.BlockSpec(memory_space=pltpu.SMEM), pl.BlockSpec(memory_space=pl.ANY)],
        out_specs=pl.BlockSpec(memory_space=pltpu.VMEM),
        scratch_shapes=[
            pltpu.VMEM((depth, group, TILE_SIZE, TILE_SIZE), jnp.bfloat16),
            pltpu.SemaphoreType.DMA((depth,)),
        ],
        out_shape=jax.ShapeDtypeStruct(slot_data.shape, jnp.bfloat16),
        compiler_params=pltpu.CompilerParams(vmem_limit_bytes=FLIP_VMEM),
        cost_estimate=pl.CostEstimate(
            flops=slots * TILE_SIZE**3,
            bytes_accessed=slots * TILE_SIZE * TILE_SIZE * 2,
            transcendentals=0,
        ),
    )(live, slot_data)


def tile_kernel(pieces, group, count_ref, rows_ref, cols_ref, tiles_ref, *refs):
    piece_refs = refs[:pieces]
    keep_ref, send_ref = refs[pieces : pieces + 2]
    panel_ref, acc_ref, piece_sems = refs[pieces + 2 :]
    halves = keep_ref.shape[0]
    per_dev = panel_ref.shape[2] // TILE_SIZE
    count = count_ref[0]
    row_at = lax.axis_index("row")
    col_at = lax.axis_index("col")
    trash = acc_ref.shape[0] - 1

    copies = [
        pltpu.make_async_copy(piece_refs[i], panel_ref.at[i], piece_sems.at[i])
        for i in range(pieces)
    ]
    for copy in copies:
        copy.start()

    @pl.loop(0, acc_ref.shape[0] // 8)
    def _(index):
        acc_ref[pl.ds(index * 8, 8)] = jnp.zeros((8,) + acc_ref.shape[1:], jnp.float32)

    for copy in copies:
        copy.wait()

    @pl.loop(0, lax.div(count + (group - 1), group))
    def _(index):
        for g in range(group):
            slot = index * group + g
            col = cols_ref[slot]
            row = jnp.where(slot < count, rows_ref[slot], trash)
            source = lax.div(col, per_dev) ^ row_at
            offset = pl.multiple_of((col & (per_dev - 1)) * TILE_SIZE, TILE_SIZE)
            picked = panel_ref[source, :, pl.ds(offset, TILE_SIZE)]
            acc_ref[row] += jnp.dot(picked, tiles_ref[slot], preferred_element_type=jnp.float32)

    pair = lax.div(col_at, 2)
    core = col_at & 1

    @pl.loop(0, halves)
    def _(h):
        base = (pair ^ h) * 2
        for ref, side in ((send_ref, 1 - core), (keep_ref, core)):
            start = (base + side) * per_dev
            for j in range(per_dev):
                ref[h, :, j * TILE_SIZE : (j + 1) * TILE_SIZE] = acc_ref[start + j].astype(
                    jnp.bfloat16
                )


def tile_products(parts, live, slot_rows, slot_cols, tiles, block_rows, halves):
    channels, nodes = parts[0].shape
    slots = slot_rows.shape[0]
    group = min(GROUP, slots)
    pieces = len(parts)
    out = jax.ShapeDtypeStruct((halves, channels, nodes), jnp.bfloat16)
    scalars = pl.BlockSpec(memory_space=pltpu.SMEM)
    vectors = pl.BlockSpec(memory_space=pltpu.VMEM)
    scratch = channels * (4 * (block_rows + 8) * TILE_SIZE + 2 * pieces * nodes)
    return pl.pallas_call(
        functools.partial(tile_kernel, pieces, group),
        in_specs=[scalars] * 3 + [vectors] + [pl.BlockSpec(memory_space=pl.ANY)] * pieces,
        out_specs=[vectors] * 2,
        scratch_shapes=[
            pltpu.VMEM((pieces, channels, nodes), jnp.bfloat16),
            pltpu.VMEM((block_rows + 8, channels, TILE_SIZE), jnp.float32),
            pltpu.SemaphoreType.DMA((pieces,)),
        ],
        out_shape=[out, out],
        compiler_params=pltpu.CompilerParams(vmem_limit_bytes=scratch + SPARE_VMEM),
        cost_estimate=pl.CostEstimate(
            flops=2 * slots * channels * TILE_SIZE * TILE_SIZE * 8,
            bytes_accessed=slots * TILE_SIZE * TILE_SIZE * 2,
            transcendentals=0,
        ),
    )(live, slot_rows, slot_cols, tiles, *parts)


def flip(size, mask):
    return [(i, i ^ mask) for i in range(size)]


def gather_masks(rows):
    masks = []
    held = [0]
    step = rows // 2
    while step:
        masks += [(mask ^ step, mask, step) for mask in reversed(held)]
        held += [mask ^ step for mask in held]
        step //= 2
    return masks


def gather_parts(own, rows):
    parts = {0: own}
    for mask, source, step in gather_masks(rows):
        parts[mask] = lax.ppermute(parts[source], "row", flip(rows, step))
    return [parts[mask] for mask in range(rows)]


def reduce_parts(keep, send, cols):
    arrived = lax.ppermute(send, "col", flip(cols, 1))
    paired = [
        (keep[half].astype(jnp.float32) + arrived[half].astype(jnp.float32)).astype(jnp.bfloat16)
        for half in range(cols // 2)
    ]
    terms = [paired[0]]
    for half in range(1, cols // 2):
        terms.append(lax.ppermute(paired[half], "col", flip(cols, 2 * half)))
    return terms


def add_terms(terms):
    total = terms[0].astype(jnp.float32)
    for term in terms[1:]:
        total = total + term.astype(jnp.float32)
    return total.astype(jnp.bfloat16)


def filter_kernel(begin, count, coef_ref, base_ref, first_ref, *refs):
    out_hbm, stage_ref, sems = refs[-3:]
    width, nodes = base_ref.shape
    strip = min(nodes, 512)

    def save(scale):
        target = out_hbm.at[scale, pl.ds(begin, width)]
        return pltpu.make_async_copy(stage_ref.at[scale], target, sems.at[scale])

    for half in range(2):
        scales = range(half * SCALES // 2, (half + 1) * SCALES // 2)

        @pl.loop(0, nodes // strip)
        def _(index):
            span = pl.ds(pl.multiple_of(index * strip, strip), strip)
            base = base_ref[:, span].astype(jnp.float32)
            first = first_ref[:, span].astype(jnp.float32)
            second = add_terms([ref[:, span] for ref in refs[:count]]).astype(jnp.float32)
            bend = 2.0 * second - base
            for scale in scales:
                stage_ref[scale, :, span] = (
                    coef_ref[0, scale] * base
                    + coef_ref[1, scale] * first
                    + coef_ref[2, scale] * bend
                ).astype(jnp.bfloat16)

        for scale in scales:
            save(scale).start()
    for scale in range(SCALES):
        save(scale).wait()


def write_filtered(coefs, base, first, terms, begin, channels, filtered):
    width, nodes = base.shape
    vectors = pl.BlockSpec(memory_space=pltpu.VMEM)
    anywhere = pl.BlockSpec(memory_space=pl.ANY)
    rest = [] if filtered is None else [filtered]
    return pl.pallas_call(
        functools.partial(filter_kernel, begin, len(terms)),
        in_specs=[pl.BlockSpec(memory_space=pltpu.SMEM)]
        + [vectors] * (2 + len(terms))
        + [anywhere] * len(rest),
        out_specs=anywhere,
        scratch_shapes=[
            pltpu.VMEM((SCALES, width, nodes), jnp.bfloat16),
            pltpu.SemaphoreType.DMA((SCALES,)),
        ],
        out_shape=jax.ShapeDtypeStruct((SCALES, channels, nodes), jnp.bfloat16),
        input_output_aliases={3 + len(terms): 0} if rest else {},
        compiler_params=pltpu.CompilerParams(vmem_limit_bytes=FILTER_VMEM),
        cost_estimate=pl.CostEstimate(
            flops=8 * SCALES * width * nodes,
            bytes_accessed=2 * SCALES * width * nodes,
            transcendentals=0,
        ),
    )(coefs, base, first, *terms, *rest)


def filter_bank(features, tile_rows, tile_cols, tile_count, tile_data):
    cols = lax.axis_size("col")
    rows = lax.axis_size("row")
    channels, nodes = features.shape
    per_dev = nodes // TILE_SIZE
    block_rows = per_dev * cols
    slot_data = tile_data.reshape(-1, TILE_SIZE, TILE_SIZE)
    live = tile_count.reshape(-1)
    slot_rows = tile_rows.reshape(-1)
    slot_cols = tile_cols.reshape(-1)

    tiles = flip_tiles(live, slot_data)

    def apply_operator(field):
        parts = gather_parts(field, rows)
        keep, send = tile_products(parts, live, slot_rows, slot_cols, tiles, block_rows, cols // 2)
        return reduce_parts(keep, send, cols)

    width = channels // CHUNKS
    coefs = jnp.stack(coefficients())
    fields = [features[i * width : (i + 1) * width] for i in range(CHUNKS)]
    firsts = []
    for field in fields:
        terms = apply_operator(field)
        firsts.append(add_terms(terms))
    seconds = [apply_operator(first) for first in firsts]
    filtered = None
    for chunk, (field, first, terms) in enumerate(zip(fields, firsts, seconds)):
        filtered = write_filtered(coefs, field, first, terms, chunk * width, channels, filtered)
    return filtered.reshape(-1, nodes)


def solution(mesh):
    return jax.shard_map(
        filter_bank,
        mesh=mesh,
        in_specs=(
            P(None, ("row", "col")),
            P("row", "col", None),
            P("row", "col", None),
            P("row", "col"),
            P("row", "col", None, None, None),
        ),
        out_specs=P(None, ("row", "col")),
        check_vma=False,
    )
```

```python
import functools

import jax
import jax.numpy as jnp
from jax import lax
from jax.experimental import pallas as pl
from jax.experimental.pallas import tpu as pltpu
from jax.sharding import PartitionSpec as P


SCALES = 8
TILE_SIZE = 128
CHUNKS = 2
GROUP = 64
FLIP_GROUP = 32
FLIP_DEPTH = 8
FLIP_VMEM = 28 * 2**20
PRODUCT_VMEM = 16 * 2**20
FILTER_VMEM = 16 * 2**20


def bessel_pair(times):
    halved = times / 2.0
    square = halved * halved
    term_zero = jnp.ones_like(times)
    term_one = halved
    sum_zero = term_zero
    sum_one = term_one
    for degree in range(1, 24):
        term_zero = term_zero * square / float(degree * degree)
        term_one = term_one * square / float(degree * (degree + 1))
        sum_zero = sum_zero + term_zero
        sum_one = sum_one + term_one
    damping = jnp.exp(-times)
    return (damping * sum_zero, damping * sum_one)


def coefficients():
    times = 0.25 * 2.0 ** (jnp.arange(SCALES).astype(jnp.float32) / 2.0)
    bessel_zero, bessel_one = bessel_pair(times)
    return (bessel_zero, -2.0 * bessel_one, 2.0 * (bessel_zero - 2.0 * bessel_one / times))


def flip_kernel(group, depth, per_dev, count_ref, rows_ref, cols_ref, tiles_hbm, *refs):
    flipped_ref, order_rows_ref, order_cols_ref, split_ref, tiles_ref, sems = refs
    slots = flipped_ref.shape[0]
    count = count_ref[0]
    row_at = lax.axis_index("row")
    last = lax.axis_size("row") - 1
    live_groups = lax.div(count + (group - 1), group)

    def load(index):
        slot = lax.rem(index, depth)
        source = tiles_hbm.at[pl.ds(index * group, group)]
        return pltpu.make_async_copy(source, tiles_ref.at[slot], sems.at[slot])

    for index in range(depth):

        @pl.when(index < live_groups)
        def _():
            load(index).start()

    def one_group(index, split):
        front, back = split
        load(index).wait()
        for g in range(group):
            slot = index * group + g
            col = cols_ref[slot]
            source = lax.div(col, per_dev) ^ row_at
            to_back = (source == last) & (slot < count)
            place = jnp.where(to_back, slots - 1 - back, front)
            flipped_ref[place] = tiles_ref[lax.rem(index, depth), g].T
            order_rows_ref[place] = rows_ref[slot]
            order_cols_ref[place] = source * per_dev + (col & (per_dev - 1))
            back = back + to_back.astype(jnp.int32)
            front = front + ((source != last) & (slot < count)).astype(jnp.int32)

        @pl.when(index + depth < live_groups)
        def _():
            load(index + depth).start()

        return front, back

    front, back = lax.fori_loop(0, live_groups, one_group, (jnp.int32(0), jnp.int32(0)))
    split_ref[0] = front
    split_ref[1] = back


def flip_tiles(live, slot_rows, slot_cols, slot_data, per_dev):
    slots = slot_data.shape[0]
    group = min(FLIP_GROUP, slots)
    depth = min(FLIP_DEPTH, slots // group)
    scalars = pl.BlockSpec(memory_space=pltpu.SMEM)
    numbers = jax.ShapeDtypeStruct((slots,), jnp.int32)
    return pl.pallas_call(
        functools.partial(flip_kernel, group, depth, per_dev),
        in_specs=[scalars] * 3 + [pl.BlockSpec(memory_space=pl.ANY)],
        out_specs=[pl.BlockSpec(memory_space=pltpu.VMEM)] + [scalars] * 3,
        scratch_shapes=[
            pltpu.VMEM((depth, group, TILE_SIZE, TILE_SIZE), jnp.bfloat16),
            pltpu.SemaphoreType.DMA((depth,)),
        ],
        out_shape=[
            jax.ShapeDtypeStruct(slot_data.shape, jnp.bfloat16),
            numbers,
            numbers,
            jax.ShapeDtypeStruct((2,), jnp.int32),
        ],
        compiler_params=pltpu.CompilerParams(vmem_limit_bytes=FLIP_VMEM),
        cost_estimate=pl.CostEstimate(
            flops=slots * TILE_SIZE**3,
            bytes_accessed=slots * TILE_SIZE * TILE_SIZE * 2,
            transcendentals=0,
        ),
    )(live, slot_rows, slot_cols, slot_data)


def front_kernel(group, split_ref, rows_ref, cols_ref, tiles_ref, *refs):
    acc_ref, panel_ref, sems = refs[-3:]
    piece_refs = refs[:-3]
    per_dev = panel_ref.shape[2] // TILE_SIZE
    trash = acc_ref.shape[0] - 1
    front = split_ref[0]
    copies = [
        pltpu.make_async_copy(ref, panel_ref.at[i], sems.at[i]) for i, ref in enumerate(piece_refs)
    ]
    for copy in copies:
        copy.start()

    @pl.loop(0, acc_ref.shape[0] // 8)
    def _(index):
        acc_ref[pl.ds(index * 8, 8)] = jnp.zeros((8,) + acc_ref.shape[1:], jnp.float32)

    for copy in copies:
        copy.wait()

    @pl.loop(0, lax.div(front + (group - 1), group))
    def _(index):
        for g in range(group):
            slot = index * group + g
            valid = slot < front
            col = jnp.where(valid, cols_ref[slot], 0)
            row = jnp.where(valid, rows_ref[slot], trash)
            offset = pl.multiple_of((col & (per_dev - 1)) * TILE_SIZE, TILE_SIZE)
            picked = panel_ref[lax.div(col, per_dev), :, pl.ds(offset, TILE_SIZE)]
            acc_ref[row] += jnp.dot(picked, tiles_ref[slot], preferred_element_type=jnp.float32)


def back_kernel(group, split_ref, rows_ref, cols_ref, tiles_ref, piece_ref, acc_in, *refs):
    acc_ref, keep_ref, send_ref = refs
    halves = keep_ref.shape[0]
    slots = tiles_ref.shape[0]
    per_dev = piece_ref.shape[1] // TILE_SIZE
    trash = acc_ref.shape[0] - 1
    back = split_ref[1]
    col_at = lax.axis_index("col")
    pair = lax.div(col_at, 2)
    core = col_at & 1

    @pl.loop(0, lax.div(back + (group - 1), group))
    def _(index):
        for g in range(group):
            slot = slots - group * (index + 1) + g
            valid = slot >= slots - back
            col = jnp.where(valid, cols_ref[slot], 0)
            row = jnp.where(valid, rows_ref[slot], trash)
            offset = pl.multiple_of((col & (per_dev - 1)) * TILE_SIZE, TILE_SIZE)
            picked = piece_ref[:, pl.ds(offset, TILE_SIZE)]
            acc_ref[row] += jnp.dot(picked, tiles_ref[slot], preferred_element_type=jnp.float32)

    @pl.loop(0, halves)
    def _(h):
        base = (pair ^ h) * 2
        for ref, side in ((send_ref, 1 - core), (keep_ref, core)):
            start = (base + side) * per_dev
            for j in range(per_dev):
                ref[h, :, j * TILE_SIZE : (j + 1) * TILE_SIZE] = acc_ref[start + j].astype(
                    jnp.bfloat16
                )


def tile_products(parts, ordered, block_rows, halves):
    tiles, slot_rows, slot_cols, split = ordered
    channels, nodes = parts[0].shape
    slots = tiles.shape[0]
    group = min(GROUP, slots)
    pieces = len(parts) - 1
    scalars = pl.BlockSpec(memory_space=pltpu.SMEM)
    vectors = pl.BlockSpec(memory_space=pltpu.VMEM)
    sums = jax.ShapeDtypeStruct((block_rows + 8, channels, TILE_SIZE), jnp.float32)
    out = jax.ShapeDtypeStruct((halves, channels, nodes), jnp.bfloat16)

    def cost(share):
        return pl.CostEstimate(
            flops=int(share * 16 * slots * channels * TILE_SIZE * TILE_SIZE),
            bytes_accessed=int(share * slots * TILE_SIZE * TILE_SIZE * 2),
            transcendentals=0,
        )

    front = pl.pallas_call(
        functools.partial(front_kernel, group),
        in_specs=[scalars] * 3 + [vectors] + [pl.BlockSpec(memory_space=pl.ANY)] * pieces,
        out_specs=vectors,
        scratch_shapes=[
            pltpu.VMEM((pieces, channels, nodes), jnp.bfloat16),
            pltpu.SemaphoreType.DMA((pieces,)),
        ],
        out_shape=sums,
        compiler_params=pltpu.CompilerParams(vmem_limit_bytes=PRODUCT_VMEM),
        cost_estimate=cost(0.7),
    )(split, slot_rows, slot_cols, tiles, *parts[:-1])
    _, keep, send = pl.pallas_call(
        functools.partial(back_kernel, group),
        in_specs=[scalars] * 3 + [vectors] * 3,
        out_specs=[vectors] * 3,
        out_shape=[sums, out, out],
        input_output_aliases={5: 0},
        compiler_params=pltpu.CompilerParams(vmem_limit_bytes=PRODUCT_VMEM),
        cost_estimate=cost(0.3),
    )(split, slot_rows, slot_cols, tiles, parts[-1], front)
    return keep, send


def flip(size, mask):
    return [(i, i ^ mask) for i in range(size)]


def gather_masks(rows):
    masks = []
    held = [0]
    step = rows // 2
    while step:
        masks += [(mask ^ step, mask, step) for mask in reversed(held)]
        held += [mask ^ step for mask in held]
        step //= 2
    return masks


def gather_parts(own, rows):
    parts = {0: own}
    for mask, source, step in gather_masks(rows):
        parts[mask] = lax.ppermute(parts[source], "row", flip(rows, step))
    return [parts[mask] for mask in range(rows)]


def reduce_parts(keep, send, cols):
    arrived = lax.ppermute(send, "col", flip(cols, 1))
    paired = [
        (keep[half].astype(jnp.float32) + arrived[half].astype(jnp.float32)).astype(jnp.bfloat16)
        for half in range(cols // 2)
    ]
    terms = [paired[0]]
    for half in range(1, cols // 2):
        terms.append(lax.ppermute(paired[half], "col", flip(cols, 2 * half)))
    return terms


def add_terms(terms):
    total = terms[0].astype(jnp.float32)
    for term in terms[1:]:
        total = total + term.astype(jnp.float32)
    return total.astype(jnp.bfloat16)


def filter_kernel(begin, count, coef_ref, base_ref, first_ref, *refs):
    out_hbm, stage_ref, sems = refs[-3:]
    width, nodes = base_ref.shape
    strip = min(nodes, 512)

    def save(scale):
        target = out_hbm.at[scale, pl.ds(begin, width)]
        return pltpu.make_async_copy(stage_ref.at[scale], target, sems.at[scale])

    for half in range(2):
        scales = range(half * SCALES // 2, (half + 1) * SCALES // 2)

        @pl.loop(0, nodes // strip)
        def _(index):
            span = pl.ds(pl.multiple_of(index * strip, strip), strip)
            base = base_ref[:, span].astype(jnp.float32)
            first = first_ref[:, span].astype(jnp.float32)
            second = add_terms([ref[:, span] for ref in refs[:count]]).astype(jnp.float32)
            bend = 2.0 * second - base
            for scale in scales:
                stage_ref[scale, :, span] = (
                    coef_ref[0, scale] * base
                    + coef_ref[1, scale] * first
                    + coef_ref[2, scale] * bend
                ).astype(jnp.bfloat16)

        for scale in scales:
            save(scale).start()
    for scale in range(SCALES):
        save(scale).wait()


def write_filtered(coefs, base, first, terms, begin, channels, filtered):
    width, nodes = base.shape
    vectors = pl.BlockSpec(memory_space=pltpu.VMEM)
    anywhere = pl.BlockSpec(memory_space=pl.ANY)
    rest = [] if filtered is None else [filtered]
    return pl.pallas_call(
        functools.partial(filter_kernel, begin, len(terms)),
        in_specs=[pl.BlockSpec(memory_space=pltpu.SMEM)]
        + [vectors] * (2 + len(terms))
        + [anywhere] * len(rest),
        out_specs=anywhere,
        scratch_shapes=[
            pltpu.VMEM((SCALES, width, nodes), jnp.bfloat16),
            pltpu.SemaphoreType.DMA((SCALES,)),
        ],
        out_shape=jax.ShapeDtypeStruct((SCALES, channels, nodes), jnp.bfloat16),
        input_output_aliases={3 + len(terms): 0} if rest else {},
        compiler_params=pltpu.CompilerParams(vmem_limit_bytes=FILTER_VMEM),
        cost_estimate=pl.CostEstimate(
            flops=8 * SCALES * width * nodes,
            bytes_accessed=2 * SCALES * width * nodes,
            transcendentals=0,
        ),
    )(coefs, base, first, *terms, *rest)


def filter_bank(features, tile_rows, tile_cols, tile_count, tile_data):
    cols = lax.axis_size("col")
    rows = lax.axis_size("row")
    channels, nodes = features.shape
    per_dev = nodes // TILE_SIZE
    block_rows = per_dev * cols
    slot_data = tile_data.reshape(-1, TILE_SIZE, TILE_SIZE)
    live = tile_count.reshape(-1)
    slot_rows = tile_rows.reshape(-1)
    slot_cols = tile_cols.reshape(-1)

    ordered = flip_tiles(live, slot_rows, slot_cols, slot_data, per_dev)

    def apply_operator(field):
        parts = gather_parts(field, rows)
        keep, send = tile_products(parts, ordered, block_rows, cols // 2)
        return reduce_parts(keep, send, cols)

    width = channels // CHUNKS
    coefs = jnp.stack(coefficients())
    fields = [features[i * width : (i + 1) * width] for i in range(CHUNKS)]
    firsts = []
    for field in fields:
        terms = apply_operator(field)
        firsts.append(add_terms(terms))
    seconds = [apply_operator(first) for first in firsts]
    filtered = None
    for chunk, (field, first, terms) in enumerate(zip(fields, firsts, seconds)):
        filtered = write_filtered(coefs, field, first, terms, chunk * width, channels, filtered)
    return filtered.reshape(-1, nodes)


def solution(mesh):
    return jax.shard_map(
        filter_bank,
        mesh=mesh,
        in_specs=(
            P(None, ("row", "col")),
            P("row", "col", None),
            P("row", "col", None),
            P("row", "col"),
            P("row", "col", None, None, None),
        ),
        out_specs=P(None, ("row", "col")),
        check_vma=False,
    )
```

```python
import functools

import jax
import jax.numpy as jnp
from jax import lax
from jax.experimental import pallas as pl
from jax.experimental.pallas import tpu as pltpu
from jax.sharding import PartitionSpec as P


SCALES = 8
TILE_SIZE = 128
CHUNKS = 2
GROUP = 64
COL_BITS = 16
COL_MASK = 2**COL_BITS - 1
FLIP_GROUP = 32
FLIP_DEPTH = 8
FLIP_VMEM = 28 * 2**20
PRODUCT_VMEM = 16 * 2**20
FILTER_VMEM = 16 * 2**20
PLAIN_VMEM = 8 * 2**20


def bessel_pair(times):
    halved = times / 2.0
    square = halved * halved
    term_zero = jnp.ones_like(times)
    term_one = halved
    sum_zero = term_zero
    sum_one = term_one
    for degree in range(1, 24):
        term_zero = term_zero * square / float(degree * degree)
        term_one = term_one * square / float(degree * (degree + 1))
        sum_zero = sum_zero + term_zero
        sum_one = sum_one + term_one
    damping = jnp.exp(-times)
    return (damping * sum_zero, damping * sum_one)


def coefficients():
    times = 0.25 * 2.0 ** (jnp.arange(SCALES).astype(jnp.float32) / 2.0)
    bessel_zero, bessel_one = bessel_pair(times)
    return (bessel_zero, -2.0 * bessel_one, 2.0 * (bessel_zero - 2.0 * bessel_one / times))


def flip_kernel(group, depth, edge, codes_ref, tiles_hbm, flipped_ref, order_ref, tiles_ref, sems):
    slots = flipped_ref.shape[0]
    count = codes_ref[slots]
    live_groups = lax.div(count + (group - 1), group)

    def load(index):
        slot = lax.rem(index, depth)
        source = tiles_hbm.at[pl.ds(index * group, group)]
        return pltpu.make_async_copy(source, tiles_ref.at[slot], sems.at[slot])

    for index in range(depth):

        @pl.when(index < live_groups)
        def _():
            load(index).start()

    def one_group(index, split):
        front, back = split
        load(index).wait()
        for g in range(group):
            slot = index * group + g
            code = codes_ref[slot]
            late = (code & COL_MASK) >= edge
            to_back = (late & (slot < count)).astype(jnp.int32)
            place = jnp.where(to_back == 1, slots - 1 - back, front)
            flipped_ref[place] = tiles_ref[lax.rem(index, depth), g].T
            order_ref[place] = code
            back = back + to_back
            front = front + (1 - to_back)

        @pl.when(index + depth < live_groups)
        def _():
            load(index + depth).start()

        return front, back

    _, back = lax.fori_loop(0, live_groups, one_group, (jnp.int32(0), jnp.int32(0)))
    order_ref[slots] = count - back
    order_ref[slots + 1] = back


def flip_tiles(codes, slot_data, edge):
    slots = slot_data.shape[0]
    group = min(FLIP_GROUP, slots)
    depth = min(FLIP_DEPTH, slots // group)
    scalars = pl.BlockSpec(memory_space=pltpu.SMEM)
    return pl.pallas_call(
        functools.partial(flip_kernel, group, depth, edge),
        in_specs=[scalars, pl.BlockSpec(memory_space=pl.ANY)],
        out_specs=[pl.BlockSpec(memory_space=pltpu.VMEM), scalars],
        scratch_shapes=[
            pltpu.VMEM((depth, group, TILE_SIZE, TILE_SIZE), jnp.bfloat16),
            pltpu.SemaphoreType.DMA((depth,)),
        ],
        out_shape=[
            jax.ShapeDtypeStruct(slot_data.shape, jnp.bfloat16),
            jax.ShapeDtypeStruct((slots + 2,), jnp.int32),
        ],
        compiler_params=pltpu.CompilerParams(vmem_limit_bytes=FLIP_VMEM),
        cost_estimate=pl.CostEstimate(
            flops=slots * TILE_SIZE**3,
            bytes_accessed=slots * TILE_SIZE * TILE_SIZE * 2,
            transcendentals=0,
        ),
    )(codes, slot_data)


def front_kernel(group, order_ref, tiles_ref, *refs):
    acc_ref, panel_ref, sems = refs[-3:]
    piece_refs = refs[:-3]
    per_dev = panel_ref.shape[2] // TILE_SIZE
    trash = acc_ref.shape[0] - 1
    front = order_ref[tiles_ref.shape[0]]
    copies = [
        pltpu.make_async_copy(ref, panel_ref.at[i], sems.at[i]) for i, ref in enumerate(piece_refs)
    ]
    for copy in copies:
        copy.start()

    @pl.loop(0, acc_ref.shape[0] // 8)
    def _(index):
        acc_ref[pl.ds(index * 8, 8)] = jnp.zeros((8,) + acc_ref.shape[1:], jnp.float32)

    for copy in copies:
        copy.wait()

    @pl.loop(0, lax.div(front + (group - 1), group))
    def _(index):
        for g in range(group):
            slot = index * group + g
            valid = slot < front
            code = jnp.where(valid, order_ref[slot], trash * (COL_MASK + 1))
            col = code & COL_MASK
            row = lax.shift_right_logical(code, COL_BITS)
            offset = pl.multiple_of((col & (per_dev - 1)) * TILE_SIZE, TILE_SIZE)
            picked = panel_ref[lax.div(col, per_dev), :, pl.ds(offset, TILE_SIZE)]
            acc_ref[row] += jnp.dot(picked, tiles_ref[slot], preferred_element_type=jnp.float32)


def back_kernel(group, order_ref, tiles_ref, piece_ref, acc_in, *refs):
    acc_ref, keep_ref, send_ref = refs
    halves = keep_ref.shape[0]
    slots = tiles_ref.shape[0]
    per_dev = piece_ref.shape[1] // TILE_SIZE
    trash = acc_ref.shape[0] - 1
    back = order_ref[slots + 1]
    col_at = lax.axis_index("col")
    pair = lax.div(col_at, 2)
    core = col_at & 1

    @pl.loop(0, lax.div(back + (group - 1), group))
    def _(index):
        for g in range(group):
            slot = slots - group * (index + 1) + g
            valid = slot >= slots - back
            code = jnp.where(valid, order_ref[slot], trash * (COL_MASK + 1))
            col = code & COL_MASK
            row = lax.shift_right_logical(code, COL_BITS)
            offset = pl.multiple_of((col & (per_dev - 1)) * TILE_SIZE, TILE_SIZE)
            picked = piece_ref[:, pl.ds(offset, TILE_SIZE)]
            acc_ref[row] += jnp.dot(picked, tiles_ref[slot], preferred_element_type=jnp.float32)

    @pl.loop(0, halves)
    def _(h):
        base = (pair ^ h) * 2
        for ref, side in ((send_ref, 1 - core), (keep_ref, core)):
            start = (base + side) * per_dev
            for j in range(per_dev):
                ref[h, :, j * TILE_SIZE : (j + 1) * TILE_SIZE] = acc_ref[start + j].astype(
                    jnp.bfloat16
                )


def tile_products(parts, ordered, block_rows, halves):
    tiles, order = ordered
    channels, nodes = parts[0].shape
    slots = tiles.shape[0]
    group = min(GROUP, slots)
    pieces = len(parts) - 1
    scalars = pl.BlockSpec(memory_space=pltpu.SMEM)
    vectors = pl.BlockSpec(memory_space=pltpu.VMEM)
    sums = jax.ShapeDtypeStruct((block_rows + 8, channels, TILE_SIZE), jnp.float32)
    out = jax.ShapeDtypeStruct((halves, channels, nodes), jnp.bfloat16)

    def cost(share):
        return pl.CostEstimate(
            flops=int(share * 16 * slots * channels * TILE_SIZE * TILE_SIZE),
            bytes_accessed=int(share * slots * TILE_SIZE * TILE_SIZE * 2),
            transcendentals=0,
        )

    front = pl.pallas_call(
        functools.partial(front_kernel, group),
        in_specs=[scalars, vectors] + [pl.BlockSpec(memory_space=pl.ANY)] * pieces,
        out_specs=vectors,
        scratch_shapes=[
            pltpu.VMEM((pieces, channels, nodes), jnp.bfloat16),
            pltpu.SemaphoreType.DMA((pieces,)),
        ],
        out_shape=sums,
        compiler_params=pltpu.CompilerParams(vmem_limit_bytes=PRODUCT_VMEM),
        cost_estimate=cost(0.7),
    )(order, tiles, *parts[:-1])
    _, keep, send = pl.pallas_call(
        functools.partial(back_kernel, group),
        in_specs=[scalars] + [vectors] * 3,
        out_specs=[vectors] * 3,
        out_shape=[sums, out, out],
        input_output_aliases={3: 0},
        compiler_params=pltpu.CompilerParams(vmem_limit_bytes=PRODUCT_VMEM),
        cost_estimate=cost(0.3),
    )(order, tiles, parts[-1], front)
    return keep, send


def flip(size, mask):
    return [(i, i ^ mask) for i in range(size)]


def gather_masks(rows):
    masks = []
    held = [0]
    step = rows // 2
    while step:
        masks += [(mask ^ step, mask, step) for mask in reversed(held)]
        held += [mask ^ step for mask in held]
        step //= 2
    return masks


def gather_parts(own, rows):
    parts = {0: own}
    for mask, source, step in gather_masks(rows):
        parts[mask] = lax.ppermute(parts[source], "row", flip(rows, step))
    return [parts[mask] for mask in range(rows)]


def reduce_parts(keep, send, cols):
    arrived = lax.ppermute(send, "col", flip(cols, 1))
    paired = [
        (keep[half].astype(jnp.float32) + arrived[half].astype(jnp.float32)).astype(jnp.bfloat16)
        for half in range(cols // 2)
    ]
    terms = [paired[0]]
    for half in range(1, cols // 2):
        terms.append(lax.ppermute(paired[half], "col", flip(cols, 2 * half)))
    return terms


def add_terms(terms):
    total = terms[0].astype(jnp.float32)
    for term in terms[1:]:
        total = total + term.astype(jnp.float32)
    return total.astype(jnp.bfloat16)


def filter_kernel(begin, count, coef_ref, plain_ref, *refs):
    out_hbm, stage_ref, sems = refs[-3:]
    width, nodes = refs[0].shape
    strip = min(nodes, 512)

    def save(scale):
        target = out_hbm.at[scale, pl.ds(begin, width)]
        return pltpu.make_async_copy(stage_ref.at[scale], target, sems.at[scale])

    for half in range(2):
        scales = range(half * SCALES // 2, (half + 1) * SCALES // 2)

        @pl.loop(0, nodes // strip)
        def _(index):
            span = pl.ds(pl.multiple_of(index * strip, strip), strip)
            second = add_terms([ref[:, span] for ref in refs[:count]]).astype(jnp.float32)
            twice = 2.0 * second
            for scale in scales:
                stage_ref[scale, :, span] = (
                    plain_ref[scale, :, span] + coef_ref[2, scale] * twice
                ).astype(jnp.bfloat16)

        for scale in scales:
            save(scale).start()
    for scale in range(SCALES):
        save(scale).wait()


def plain_kernel(coef_ref, base_ref, first_ref, plain_ref):
    strip = min(base_ref.shape[1], 512)

    @pl.loop(0, base_ref.shape[1] // strip)
    def _(index):
        span = pl.ds(pl.multiple_of(index * strip, strip), strip)
        base = base_ref[:, span].astype(jnp.float32)
        first = first_ref[:, span].astype(jnp.float32)
        for scale in range(SCALES):
            plain_ref[scale, :, span] = (
                coef_ref[0, scale] - coef_ref[2, scale]
            ) * base + coef_ref[1, scale] * first


def plain_part(coefs, base, first):
    width, nodes = base.shape
    vectors = pl.BlockSpec(memory_space=pltpu.VMEM)
    return pl.pallas_call(
        plain_kernel,
        in_specs=[pl.BlockSpec(memory_space=pltpu.SMEM)] + [vectors] * 2,
        out_specs=vectors,
        out_shape=jax.ShapeDtypeStruct((SCALES, width, nodes), jnp.float32),
        compiler_params=pltpu.CompilerParams(vmem_limit_bytes=PLAIN_VMEM),
        cost_estimate=pl.CostEstimate(
            flops=4 * SCALES * width * nodes,
            bytes_accessed=4 * SCALES * width * nodes,
            transcendentals=0,
        ),
    )(coefs, base, first)


def write_filtered(coefs, plain, terms, begin, channels, filtered):
    width, nodes = terms[0].shape
    vectors = pl.BlockSpec(memory_space=pltpu.VMEM)
    anywhere = pl.BlockSpec(memory_space=pl.ANY)
    rest = [] if filtered is None else [filtered]
    return pl.pallas_call(
        functools.partial(filter_kernel, begin, len(terms)),
        in_specs=[pl.BlockSpec(memory_space=pltpu.SMEM)]
        + [vectors] * (1 + len(terms))
        + [anywhere] * len(rest),
        out_specs=anywhere,
        scratch_shapes=[
            pltpu.VMEM((SCALES, width, nodes), jnp.bfloat16),
            pltpu.SemaphoreType.DMA((SCALES,)),
        ],
        out_shape=jax.ShapeDtypeStruct((SCALES, channels, nodes), jnp.bfloat16),
        input_output_aliases={2 + len(terms): 0} if rest else {},
        compiler_params=pltpu.CompilerParams(vmem_limit_bytes=FILTER_VMEM),
        cost_estimate=pl.CostEstimate(
            flops=8 * SCALES * width * nodes,
            bytes_accessed=2 * SCALES * width * nodes,
            transcendentals=0,
        ),
    )(coefs, plain, *terms, *rest)


def filter_bank(features, tile_rows, tile_cols, tile_count, tile_data):
    cols = lax.axis_size("col")
    rows = lax.axis_size("row")
    channels, nodes = features.shape
    per_dev = nodes // TILE_SIZE
    block_rows = per_dev * cols
    slot_data = tile_data.reshape(-1, TILE_SIZE, TILE_SIZE)
    slot_cols = tile_cols.reshape(-1)
    source = (slot_cols // per_dev) ^ lax.axis_index("row")
    codes = tile_rows.reshape(-1) * (COL_MASK + 1) + source * per_dev + slot_cols % per_dev
    codes = jnp.concatenate([codes, tile_count.reshape(-1)])

    ordered = flip_tiles(codes, slot_data, (rows - 1) * per_dev)

    def apply_operator(field):
        parts = gather_parts(field, rows)
        keep, send = tile_products(parts, ordered, block_rows, cols // 2)
        return reduce_parts(keep, send, cols)

    width = channels // CHUNKS
    coefs = jnp.stack(coefficients())
    fields = [features[i * width : (i + 1) * width] for i in range(CHUNKS)]
    firsts = []
    for field in fields:
        terms = apply_operator(field)
        firsts.append(add_terms(terms))
    seconds = [apply_operator(first) for first in firsts]
    filtered = None
    for chunk, (field, first, terms) in enumerate(zip(fields, firsts, seconds)):
        plain = plain_part(coefs, field, first)
        filtered = write_filtered(coefs, plain, terms, chunk * width, channels, filtered)
    return filtered.reshape(-1, nodes)


def solution(mesh):
    return jax.shard_map(
        filter_bank,
        mesh=mesh,
        in_specs=(
            P(None, ("row", "col")),
            P("row", "col", None),
            P("row", "col", None),
            P("row", "col"),
            P("row", "col", None, None, None),
        ),
        out_specs=P(None, ("row", "col")),
        check_vma=False,
    )
```
